128 devices in a mesh: comp: 16 (over y, z_hi, core), gx: 2 (over z_lo), gy: 4 (over x).
Axes of the slice: x: 4, y: 4, z: 4 (z_hi: 2, z_lo: 2; z = z_hi * 2 + z_lo), core: 2. Of those that a mesh axis runs over, the one named last changes fastest.
Arguments:
- field: float32 [16, 256, 64, 256], P('comp', 'gx', 'gy'), may hold values from -6 to 6
- third_level: int32 [16], replicated, may hold values from 2 to 6
- coefficients: int32 [16], replicated, may hold values from -3 to 3, as said below
- rates: float32 [2, 4], replicated, may hold values from 0.01 to 0.4, as said below
- reaction: float32 [1], replicated, may hold values from 0.1 to 0.3
Outputs:
- result: float32 [16, 256, 64, 256], P('comp', 'gx', 'gy')
The draws below stay inside these ranges and needn't reach their ends.
Inputs may be any that keep to these rules, and one draw needn't show every extreme that they name: The fourth dimension of grid g has level 8 minus third_level[g]. `coefficients`: every weight is a nonzero integer; some are positive and some negative. `rates`: courant numbers of the first two dimensions lie from 0.3 to 0.4, all other entries from 0.01 to 0.02.
All inputs are finite; a program needn't handle non-finite values.
Results may differ from the reference program's by a relative error of at most 0.0003.
Values sent between devices are 32-bit elements; how exact they have to be, the bound alone decides.
A program may use at most 128 MiB of HBM per device.

```python
import math
import jax
import jax.numpy as jnp
import numpy as np
from jax import lax

SECTIONS = 4
LEVEL_SUM = 8
FLAT = 256
GRIDS = 16
NX = 256
NY = 64


def draw_coefficients(key, part):
    magnitude = jax.random.randint(jax.random.fold_in(key, 11), (GRIDS,), 1, 4)
    signs = 2 * jax.random.randint(jax.random.fold_in(key, 12), (GRIDS,), 0, 2) - 1
    order = jax.random.permutation(jax.random.fold_in(key, 13), GRIDS)
    signs = signs.at[order[0]].set(1)
    signs = signs.at[order[1]].set(-1)
    magnitude = magnitude.at[order[0]].set(3)
    magnitude = magnitude.at[order[1]].set(3)
    return (signs * magnitude).astype(jnp.int32)


def draw_rates(key, part):
    base = jax.random.uniform(jax.random.fold_in(key, 7), (2, 4), jnp.float32)
    lower = jnp.array([[0.01, 0.01, 0.01, 0.01], [0.3, 0.3, 0.01, 0.01]], jnp.float32)
    spread = jnp.array([[0.01, 0.01, 0.01, 0.01], [0.1, 0.1, 0.01, 0.01]], jnp.float32)
    return (lower + spread * base).astype(jnp.float32)


def plant(result, rng, least, top_value):
    dims = result.shape
    spot = [jax.random.randint(jax.random.fold_in(rng, axis), (), 0, dims[axis]) for axis in range(len(dims))]
    result = result.at[tuple(spot)].set(least)
    longest = dims.index(max(dims))
    spot[longest] = (spot[longest] + 1) % dims[longest]
    return result.at[tuple(spot)].set(top_value)


def shard_levels(rng, dims, shards, least, high):
    def one(dim, shards_of):
        heights = jax.random.uniform(jax.random.fold_in(jax.random.fold_in(rng, 6), dim), (shards_of,), jnp.float32, least / len(shards), high / len(shards))
        return jnp.repeat(jnp.exp(heights), dims[dim] // shards_of).reshape((-1,) + (1,) * (len(dims) - dim - 1))

    level = one(*shards[0])
    for cut in shards[1:]:
        level = level * one(*cut)
    return level


def normal_values(rng, extent, scale, bound, pieces=(), held_as=jnp.bfloat16):
    entries = jax.random.normal(rng, extent, jnp.float32) * scale
    if len(pieces) > 0:
        entries = shard_levels(rng, extent, pieces, -0.22, 0.18) * entries
    return jnp.clip(entries, min=-bound, max=bound).astype(held_as)


def setup_inputs(seed: int = 0) -> dict:
    key_list = jax.random.split(jax.random.key(seed), 6)
    return {
        "field": normal_values(key_list[0], (GRIDS, NX, NY, FLAT), 1.0, 6.0, ((0, 16), (1, 2), (2, 4)), jnp.float32),
        "third_level": plant(jax.random.randint(key_list[1], (GRIDS,), 2, LEVEL_SUM - 1), jax.random.fold_in(key_list[1], 1), 2, (LEVEL_SUM - 1) - 1).astype(jnp.int32),
        "coefficients": draw_coefficients(jax.random.fold_in(key_list[5], 71), 0),
        "rates": draw_rates(jax.random.fold_in(key_list[5], 71), 0),
        "reaction": jnp.clip(jnp.exp(jax.random.uniform(key_list[4], (1,), jnp.float32, math.log(0.1), math.log(0.3))), 0.1, 0.3),
    }


def points(level):
    return 1 if level == 0 else 2 ** (level - 1)


def slot_table():
    top = LEVEL_SUM - 2
    table = np.zeros((top + 1) * (top + 1), np.int32)
    total = 0
    for first in range(top + 1):
        for second in range(top + 1):
            if first + second <= LEVEL_SUM:
                table[first * (top + 1) + second] = total
                total += points(first) * points(second)
    return table, total


def hier_level(index, level):
    zeros = jnp.zeros_like(index)
    for power in range(1, LEVEL_SUM + 1):
        zeros = zeros + (jnp.remainder(index, 2 ** power) == 0).astype(jnp.int32)
    depth = jnp.where(index == 0, 0, level - zeros).astype(jnp.int32)
    placed = jnp.where(index == 0, 0, jnp.right_shift(index, zeros + 1)).astype(jnp.int32)
    return depth, placed


def fast_layout(level_a, size):
    level_b = LEVEL_SUM - level_a
    width = jnp.left_shift(jnp.int32(1), level_b)
    index = jnp.arange(size, dtype=jnp.int32)
    third = index // width
    return width, third, index - third * width


def slot_positions(level_a, table):
    top = LEVEL_SUM - 2
    size = 2 ** LEVEL_SUM
    width, third, fourth = fast_layout(level_a, size)
    depth_third, rank_third = hier_level(third, level_a)
    depth_fourth, rank_fourth = hier_level(fourth, LEVEL_SUM - level_a)
    count_fourth = jnp.where(depth_fourth == 0, 1, jnp.left_shift(jnp.int32(1), jnp.maximum(depth_fourth - 1, 0)))
    code = depth_third * (top + 1) + depth_fourth
    choose = code[:, None] == jnp.arange((top + 1) * (top + 1), dtype=jnp.int32)[None, :]
    offset = jnp.sum(jnp.where(choose, jnp.asarray(table)[None, :], 0), axis=1).astype(jnp.int32)
    return offset + rank_third * count_fourth + rank_fourth


def block_neighbours(values, shift, width, inner):
    ahead = jnp.where(inner + shift < width, jnp.roll(values, -shift, axis=-1), jnp.roll(values, width - shift, axis=-1))
    behind = jnp.where(inner - shift >= 0, jnp.roll(values, shift, axis=-1), jnp.roll(values, shift - width, axis=-1))
    return ahead, behind


def transform(values, level_a, forward):
    top = LEVEL_SUM - 2
    level_b = LEVEL_SUM - level_a
    width, third, fourth = fast_layout(level_a, values.shape[-1])
    depth_third = hier_level(third, level_a)[0]
    depth_fourth = hier_level(fourth, level_b)[0]
    factor = -0.5 if forward else 0.5

    def fourth_pass(values, level):
        shift = jnp.left_shift(jnp.int32(1), jnp.maximum(level_b - level, 0))
        ahead, behind = block_neighbours(values, shift, width, fourth)
        return jnp.where(depth_fourth == level, values + factor * (ahead + behind), values)

    def third_pass(values, level):
        shift = jnp.left_shift(jnp.int32(1), jnp.maximum(level_a - level, 0))
        ahead = jnp.roll(values, -shift * width, axis=-1)
        behind = jnp.roll(values, shift * width, axis=-1)
        return jnp.where(depth_third == level, values + factor * (ahead + behind), values)

    if forward:
        for level in range(top, 0, -1):
            values = fourth_pass(values, level)
        for level in range(top, 0, -1):
            values = third_pass(values, level)
    else:
        for level in range(1, top + 1):
            values = third_pass(values, level)
        for level in range(1, top + 1):
            values = fourth_pass(values, level)
    return values


def grid_rates(rates, level_a):
    top = LEVEL_SUM - 2
    level_b = LEVEL_SUM - level_a
    coarse_third = 1.0 / jnp.left_shift(jnp.int32(1), top - level_a).astype(jnp.float32)
    coarse_fourth = 1.0 / jnp.left_shift(jnp.int32(1), top - level_b).astype(jnp.float32)
    unity = jnp.ones((), jnp.float32)
    diffusion = rates[0] * jnp.stack([unity, unity, coarse_third * coarse_third, coarse_fourth * coarse_fourth])
    courant = rates[1] * jnp.stack([unity, unity, coarse_third, coarse_fourth])
    return diffusion, courant


def advance(padded, diffusion, courant, rate, width, fourth):
    centre = padded[1:-1, 1:-1]
    up_first = padded[2:, 1:-1]
    down_first = padded[:-2, 1:-1]
    up_second = padded[1:-1, 2:]
    down_second = padded[1:-1, :-2]
    up_third = jnp.roll(centre, -width, axis=-1)
    down_third = jnp.roll(centre, width, axis=-1)
    up_fourth, down_fourth = block_neighbours(centre, 1, width, fourth)
    change = diffusion[0] * (up_first - 2.0 * centre + down_first) - courant[0] * (centre - down_first)
    change = change + diffusion[1] * (up_second - 2.0 * centre + down_second) - courant[1] * (centre - down_second)
    change = change + diffusion[2] * (up_third - 2.0 * centre + down_third) - courant[2] * (centre - down_third)
    change = change + diffusion[3] * (up_fourth - 2.0 * centre + down_fourth) - courant[3] * (centre - down_fourth)
    return centre + change + rate * centre / (1.0 + centre * centre)


def reference(field, third_level, coefficients, rates, reaction):
    table, total_slots = slot_table()
    grids = jnp.arange(GRIDS, dtype=jnp.int32)

    def evolve(grid):
        values = field[grid]
        level_a = third_level[grid]
        diffusion, courant = grid_rates(rates, level_a)
        width, third, fourth = fast_layout(level_a, values.shape[-1])
        for section in range(SECTIONS):
            padded = jnp.pad(values, ((1, 1), (1, 1), (0, 0)), mode="wrap")
            values = advance(padded, diffusion, courant, reaction[0], width, fourth)
        return transform(values, level_a, True) * coefficients[grid].astype(jnp.float32)

    surplus = lax.map(evolve, grids)

    def accumulate(total, grid):
        slots = slot_positions(third_level[grid], table)
        return total.at[:, :, slots].add(surplus[grid]), None

    combined, unused = lax.scan(accumulate, jnp.zeros((NX, NY, total_slots), jnp.float32), grids)

    def finish(grid):
        level_a = third_level[grid]
        mine = jnp.take(combined, slot_positions(level_a, table), axis=-1)
        return transform(mine, level_a, False)

    return lax.map(finish, grids)
```

```python
import functools

import jax
import jax.numpy as jnp
import ml_dtypes
import numpy as np
from jax import lax
from jax.experimental import pallas as pl
from jax.experimental.pallas import tpu as pltpu
from jax.sharding import PartitionSpec as P

MESH = pl.DeviceIdType.MESH
SECTIONS = 4
LEVEL_SUM = 8
LEVELS = (2, 3, 4, 5, 6)
FLAT = 256
GRIDS = 16
CHUNKS = 4
ORDER = [(1, 0), (0, 1), (3, 0), (1, 1), (2, 0), (3, 1), (2, 1)]
PEERS = [(y, z, c) for y, z in ORDER for c in (0, 1)] + [(0, 0, 1)]


def hat_matrix(fine, coarse):
    step = 2 ** (fine - coarse)
    count = 2**coarse
    out = np.zeros((2**fine, count), np.float64)
    for i in range(2**fine):
        left, part = divmod(i, step)
        out[i, left] += 1 - part / step
        out[i, (left + 1) % count] += part / step
    return out


def pick_matrix(coarse, fine):
    out = np.zeros((2**coarse, 2**fine), np.float64)
    out[np.arange(2**coarse), np.arange(2**coarse) * 2 ** (fine - coarse)] = 1
    return out


def between(low, high):
    return pick_matrix(low, high) if low <= high else hat_matrix(low, high)


def exchange_matrix(to, source):
    third = between(to, source)
    fourth = between(LEVEL_SUM - to, LEVEL_SUM - source)
    return np.kron(third, fourth).T


def exchange_table():
    out = np.stack(
        [
            np.concatenate([exchange_matrix(to, source) for source in LEVELS if source != to])
            for to in LEVELS
        ]
    )
    return out.astype(ml_dtypes.bfloat16)


def split(values):
    high = values.astype(jnp.bfloat16)
    return high, (values - high.astype(jnp.float32)).astype(jnp.bfloat16)


def dot(a, b):
    return jnp.dot(a, b, preferred_element_type=jnp.float32)


def kernel(
    field, table, level_ref, coef_ref, rate_ref, react_ref,
    out,
    u0, up8, dn8, ta, tb, mm, a_hi, a_lo, sent, got, lvl, res, back, tab,
    load_sem, tab_sem, hs_sem, hr_sem, s1, r1, s2, r2,
):
    rows = field.shape[0]
    cy = field.shape[1]
    per = rows // CHUNKS
    own = per // GRIDS
    comp, gx, gy = (lax.axis_index(a) for a in ("comp", "gx", "gy"))
    y, z, c = comp // 4, (comp // 2) % 2, comp % 2

    def mate(p, sign=1):
        return ((y + sign * p[0]) % 4) * 4 + ((z + p[1]) % 2) * 2 + (c + p[2]) % 2

    loads = [
        pltpu.make_async_copy(
            field.at[pl.ds(k * per, per)],
            u0.at[pl.ds(4 + k * per, per), pl.ds(0, cy)],
            load_sem.at[k],
        )
        for k in range(CHUNKS)
    ]
    for copy in loads:
        copy.start()
    tab_copy = pltpu.make_async_copy(table, tab, tab_sem)
    tab_copy.start()

    gxo = (gx + 1) % 2
    gyu, gyd = (gy + 1) % 4, (gy + 3) % 4
    near = [
        {"gx": gxo},
        {"gy": gyu},
        {"gy": gyd},
        {"gx": gxo, "gy": gyu},
        {"gx": gxo, "gy": gyd},
    ]
    barrier = pltpu.get_barrier_semaphore()
    for device in near + [{"comp": mate(p)} for p in PEERS]:
        pl.semaphore_signal(barrier, inc=1, device_id=device, device_id_type=MESH)

    level = level_ref[comp]
    coarse3 = jnp.float32(1.0)
    coarse4 = jnp.float32(1.0)
    for a in LEVELS:
        coarse3 = jnp.where(level == a, jnp.float32(2.0 ** (a - 6)), coarse3)
        coarse4 = jnp.where(level == a, jnp.float32(2.0 ** (2 - a)), coarse4)
    d0, d1 = rate_ref[0, 0], rate_ref[0, 1]
    d2, d3 = rate_ref[0, 2] * (coarse3 * coarse3), rate_ref[0, 3] * (coarse4 * coarse4)
    q0, q1 = rate_ref[1, 0], rate_ref[1, 1]
    q2, q3 = rate_ref[1, 2] * coarse3, rate_ref[1, 3] * coarse4
    rate = react_ref[0]
    keep = 1.0 - 2.0 * (d0 + d1 + d2 + d3) - (q0 + q1 + q2 + q3)
    width = jnp.int32(1)
    for a in LEVELS:
        width = jnp.where(level == a, jnp.int32(2 ** (LEVEL_SUM - a)), width)

    def neighbours(t, carry):
        at = t * 8 + lax.broadcasted_iota(jnp.int32, (8, FLAT), 0)
        to = lax.broadcasted_iota(jnp.int32, (8, FLAT), 1)
        inner = jnp.bitwise_and(to, width - 1)
        base = to - inner
        value = jnp.where(at == jnp.bitwise_and(to + width, FLAT - 1), d2, 0.0)
        value += jnp.where(at == jnp.bitwise_and(to - width, FLAT - 1), d2 + q2, 0.0)
        value += jnp.where(at == base + jnp.bitwise_and(inner + 1, width - 1), d3, 0.0)
        value += jnp.where(at == base + jnp.bitwise_and(inner - 1, width - 1), d3 + q3, 0.0)
        mm[pl.ds(t * 8, 8)] = value
        return carry

    lax.fori_loop(0, FLAT // 8, neighbours, 0)
    high, low = split(mm[pl.ds(0, FLAT)])
    a_hi[...] = high
    a_lo[...] = low

    for copy in loads:
        copy.wait()
    pl.semaphore_wait(barrier, len(near) + len(PEERS))

    def send(i, src, dst, device):
        copy = pltpu.make_async_remote_copy(
            src, dst, hs_sem.at[i], hr_sem.at[i], device_id=device, device_id_type=MESH
        )
        copy.start()
        return copy

    lo_tile, hi_tile = pl.ds(0, 8), pl.ds(cy - 8, 8)
    first, last = pl.ds(4, 4), pl.ds(rows, 4)
    before, after = pl.ds(0, 4), pl.ds(rows + 4, 4)
    body = pl.ds(0, cy)
    head = [
        send(0, u0.at[last, body], u0.at[before, body], {"gx": gxo}),
        send(1, u0.at[last, lo_tile], up8.at[before], {"gx": gxo, "gy": gyd}),
        send(2, u0.at[last, hi_tile], dn8.at[before], {"gx": gxo, "gy": gyu}),
    ]
    tail = [
        send(3, u0.at[first, body], u0.at[after, body], {"gx": gxo}),
        send(4, u0.at[first, lo_tile], up8.at[after], {"gx": gxo, "gy": gyd}),
        send(5, u0.at[first, hi_tile], dn8.at[after], {"gx": gxo, "gy": gyu}),
    ]
    sides = []
    for k in range(CHUNKS):
        begin = 4 if k == 0 else 8 + k * per
        end = rows + 4 if k == CHUNKS - 1 else 8 + (k + 1) * per
        part = pl.ds(begin, end - begin)
        sides.append(
            [
                send(6 + 2 * k, u0.at[part, lo_tile], up8.at[part], {"gy": gyd}),
                send(7 + 2 * k, u0.at[part, hi_tile], dn8.at[part], {"gy": gyu}),
            ]
        )

    def section(src, src_first, dst, count, final):
        def block(b, carry):
            r0 = src_first + b * 8
            flat = src[pl.ds(r0, 8)].reshape(8 * 24, FLAT)
            high, low = split(flat)
            mm[pl.ds(0, 192)] = dot(high, a_hi[...]) + dot(low, a_hi[...]) + dot(high, a_lo[...])
            for i in range(8):
                centre = src[r0 + i]
                above, below = src[r0 + i + 1], src[r0 + i - 1]
                value = (keep + rate / (1.0 + centre * centre)) * centre
                value += d0 * above + (d0 + q0) * below
                value += d1 * pltpu.roll(centre, 23, 0) + (d1 + q1) * pltpu.roll(centre, 1, 0)
                value += mm[pl.ds(i * 24, 24)]
                if final is None:
                    dst[b * 8 + i] = value
                else:
                    dst[final + b * 8 + i] = value[:cy]
            return carry

        lax.fori_loop(0, count // 8, block, 0)

    def forward(k):
        def copy(i, p, device):
            return pltpu.make_async_remote_copy(
                sent.at[pl.ds(k * per + device * own, own)],
                got.at[k, comp],
                s1.at[k, i],
                r1.at[k, i],
                device_id={"comp": device},
                device_id_type=MESH,
            )

        return [copy(i, p, mate(p)) for i, p in enumerate(PEERS)]

    def backward(k):
        def copy(i, p, device):
            return pltpu.make_async_remote_copy(
                back.at[k, device],
                out.at[pl.ds(k * per + comp * own, own)],
                s2.at[k, i],
                r2.at[k, i],
                device_id={"comp": device},
                device_id_type=MESH,
            )

        return [copy(i, p, mate(p)) for i, p in enumerate(PEERS)]

    lane_low = lax.broadcasted_iota(jnp.int32, (8, FLAT), 0) < 4

    def stencil(k):
        def halo(t, carry):
            r = k * per + t
            u0[r, pl.ds(cy, 8)] = jnp.where(lane_low, up8[r], dn8[r])
            return carry

        lax.fori_loop(0, per + 8, halo, 0)
        section(u0, k * per + 1, ta, per + 6 + 2, None)
        section(ta, 1, tb, per + 4 + 4, None)
        section(tb, 1, ta, per + 2 + 6, None)
        section(ta, 1, sent, per, k * per)

    flat_rows = own * cy

    def place(a):
        return jnp.clip(a - LEVELS[0], 0, len(LEVELS) - 1)

    def combine(k):
        for copy in forward(k):
            copy.wait_recv()
        got[k, comp] = sent[pl.ds(k * per + comp * own, own)]
        for n, a in enumerate(LEVELS):
            total = jnp.zeros((own, cy, FLAT), jnp.float32)
            for g in range(GRIDS):
                weight = jnp.where(level_ref[g] == a, coef_ref[g], 0).astype(jnp.float32)
                total += weight * got[k, g]
            total = total.reshape(flat_rows, FLAT)
            res[n] = total
            high, low = split(total)
            lvl[n, pl.ds(0, flat_rows)] = high
            lvl[n, pl.ds(flat_rows, flat_rows)] = low
        for n, a in enumerate(LEVELS):
            value = jnp.zeros((2 * flat_rows, FLAT), jnp.float32)
            for m, other in enumerate([o for o in range(len(LEVELS)) if o != n]):
                value += dot(lvl[other], tab[n, pl.ds(m * FLAT, FLAT)])
            res[n] += value[:flat_rows] + value[flat_rows:]
        for g in range(GRIDS):
            back[k, g] = res[place(level_ref[g])].reshape(own, cy, FLAT)
        out[pl.ds(k * per + comp * own, own)] = res[place(level)].reshape(own, cy, FLAT)
        for copy in backward(k):
            copy.start()

    for k in range(CHUNKS):
        for copy in sides[k]:
            copy.wait_recv()
        if k == 0:
            for copy in head:
                copy.wait_recv()
        if k == CHUNKS - 1:
            for copy in tail:
                copy.wait_recv()
        stencil(k)
        for copy in forward(k):
            copy.start()
        if k == 0:
            tab_copy.wait()
        else:
            combine(k - 1)
    combine(CHUNKS - 1)
    for copy in head + tail + sum(sides, []):
        copy.wait_send()
    for k in range(CHUNKS):
        for copy in forward(k):
            copy.wait_send()
        for copy in backward(k):
            copy.wait()


def solution(mesh):
    table = exchange_table()

    def local(field, third_level, coefficients, rates, reaction):
        _, rows, cy, flat = field.shape
        per = rows // CHUNKS
        own = per // GRIDS
        vmem, smem, anys = (
            pl.BlockSpec(memory_space=m) for m in (pltpu.VMEM, pltpu.SMEM, pl.ANY)
        )
        f32, bf16 = jnp.float32, jnp.bfloat16
        dma = pltpu.SemaphoreType.DMA
        peers = len(PEERS)
        halos = 6 + 2 * CHUNKS
        result = pl.pallas_call(
            kernel,
            out_shape=jax.ShapeDtypeStruct((rows, cy, flat), f32),
            in_specs=[anys, anys, smem, smem, smem, smem],
            out_specs=vmem,
            scratch_shapes=[
                pltpu.VMEM((rows + 8 + 8, cy + 8, flat), f32),
                pltpu.VMEM((rows + 8, 8, flat), f32),
                pltpu.VMEM((rows + 8, 8, flat), f32),
                pltpu.VMEM((per + 16, cy + 8, flat), f32),
                pltpu.VMEM((per + 16, cy + 8, flat), f32),
                pltpu.VMEM((max(8 * (cy + 8), flat), flat), f32),
                pltpu.VMEM((flat, flat), bf16),
                pltpu.VMEM((flat, flat), bf16),
                pltpu.VMEM((rows, cy, flat), f32),
                pltpu.VMEM((CHUNKS, GRIDS, own, cy, flat), f32),
                pltpu.VMEM((len(LEVELS), 2 * own * cy, flat), bf16),
                pltpu.VMEM((len(LEVELS), own * cy, flat), f32),
                pltpu.VMEM((CHUNKS, GRIDS, own, cy, flat), f32),
                pltpu.VMEM(table.shape, bf16),
                dma((CHUNKS,)),
                dma,
                dma((halos,)),
                dma((halos,)),
                dma((CHUNKS, peers)),
                dma((CHUNKS, peers)),
                dma((CHUNKS, peers)),
                dma((CHUNKS, peers)),
            ],
            compiler_params=pltpu.CompilerParams(
                collective_id=0, has_side_effects=True, vmem_limit_bytes=40 << 20
            ),
        )(field[0], jnp.asarray(table), third_level, coefficients, rates, reaction)
        return result[None]

    return jax.shard_map(
        local,
        mesh=mesh,
        in_specs=(P("comp", "gx", "gy", None), P(), P(), P(), P()),
        out_specs=P("comp", "gx", "gy", None),
        check_vma=False,
    )
```

```python
import functools

import jax
import jax.numpy as jnp
import ml_dtypes
import numpy as np
from jax import lax
from jax.experimental import pallas as pl
from jax.experimental.pallas import tpu as pltpu
from jax.sharding import PartitionSpec as P

MESH = pl.DeviceIdType.MESH
SECTIONS = 4
LEVEL_SUM = 8
LEVELS = (2, 3, 4, 5, 6)
FLAT = 256
GRIDS = 16
CHUNKS = 4
ORDER = [(1, 0), (0, 1), (3, 0), (1, 1), (2, 0), (3, 1), (2, 1)]
PEERS = [(y, z, c) for y, z in ORDER for c in (0, 1)] + [(0, 0, 1)]


def hat_matrix(fine, coarse):
    step = 2 ** (fine - coarse)
    count = 2**coarse
    out = np.zeros((2**fine, count), np.float64)
    for i in range(2**fine):
        left, part = divmod(i, step)
        out[i, left] += 1 - part / step
        out[i, (left + 1) % count] += part / step
    return out


def pick_matrix(coarse, fine):
    out = np.zeros((2**coarse, 2**fine), np.float64)
    out[np.arange(2**coarse), np.arange(2**coarse) * 2 ** (fine - coarse)] = 1
    return out


def between(low, high):
    return pick_matrix(low, high) if low <= high else hat_matrix(low, high)


def exchange_matrix(to, source):
    third = between(to, source)
    fourth = between(LEVEL_SUM - to, LEVEL_SUM - source)
    return np.kron(third, fourth).T


def exchange_table():
    out = np.stack(
        [
            np.concatenate([exchange_matrix(to, source) for source in LEVELS if source != to])
            for to in LEVELS
        ]
    )
    return out.astype(ml_dtypes.bfloat16)


def split(values):
    high = values.astype(jnp.bfloat16)
    return high, (values - high.astype(jnp.float32)).astype(jnp.bfloat16)


def dot(a, b):
    return jnp.dot(a, b, preferred_element_type=jnp.float32)


def kernel(
    field, table, level_in, coef_in, rate_in, react_in,
    out,
    level_ref, coef_ref, rate_ref, react_ref, small_sem,
    u0, pack_up, pack_dn, up8, dn8, ta, tb, mm, a_hi, a_lo, sent, got, lvl, res, back, tab,
    load_sem, tab_sem, hs_sem, hr_sem, s1, r1, s2, r2,
):
    rows = field.shape[0]
    cy = field.shape[1]
    per = rows // CHUNKS
    own = per // GRIDS
    comp, gx, gy = (lax.axis_index(a) for a in ("comp", "gx", "gy"))
    y, z, c = comp // 4, (comp // 2) % 2, comp % 2

    def mate(p, sign=1):
        return ((y + sign * p[0]) % 4) * 4 + ((z + p[1]) % 2) * 2 + (c + p[2]) % 2

    loads = [
        pltpu.make_async_copy(
            field.at[pl.ds(k * per, per)],
            u0.at[pl.ds(4 + k * per, per), pl.ds(0, cy)],
            load_sem.at[k],
        )
        for k in range(CHUNKS)
    ]
    smalls = [
        pltpu.make_async_copy(src, dst, small_sem.at[i])
        for i, (src, dst) in enumerate(
            [(level_in, level_ref), (rate_in, rate_ref), (react_in, react_ref), (coef_in, coef_ref)]
        )
    ]
    for copy in smalls + loads:
        copy.start()
    tab_copy = pltpu.make_async_copy(table, tab, tab_sem)
    tab_copy.start()

    gxo = (gx + 1) % 2
    gyu, gyd = (gy + 1) % 4, (gy + 3) % 4
    near = [
        {"gx": gxo},
        {"gy": gyu},
        {"gy": gyd},
        {"gx": gxo, "gy": gyu},
        {"gx": gxo, "gy": gyd},
    ]
    barrier = pltpu.get_barrier_semaphore()
    for device in near + [{"comp": mate(p)} for p in PEERS]:
        pl.semaphore_signal(barrier, inc=1, device_id=device, device_id_type=MESH)

    for copy in smalls:
        copy.wait()
    level = level_ref[comp]
    coarse3 = jnp.float32(1.0)
    coarse4 = jnp.float32(1.0)
    for a in LEVELS:
        coarse3 = jnp.where(level == a, jnp.float32(2.0 ** (a - 6)), coarse3)
        coarse4 = jnp.where(level == a, jnp.float32(2.0 ** (2 - a)), coarse4)
    d0, d1 = rate_ref[0, 0], rate_ref[0, 1]
    d2, d3 = rate_ref[0, 2] * (coarse3 * coarse3), rate_ref[0, 3] * (coarse4 * coarse4)
    q0, q1 = rate_ref[1, 0], rate_ref[1, 1]
    q2, q3 = rate_ref[1, 2] * coarse3, rate_ref[1, 3] * coarse4
    rate = react_ref[0]
    keep = 1.0 - 2.0 * (d0 + d1 + d2 + d3) - (q0 + q1 + q2 + q3)
    width = jnp.int32(1)
    for a in LEVELS:
        width = jnp.where(level == a, jnp.int32(2 ** (LEVEL_SUM - a)), width)

    def neighbours(t, carry):
        at = t * 8 + lax.broadcasted_iota(jnp.int32, (8, FLAT), 0)
        to = lax.broadcasted_iota(jnp.int32, (8, FLAT), 1)
        inner = jnp.bitwise_and(to, width - 1)
        base = to - inner
        value = jnp.where(at == jnp.bitwise_and(to + width, FLAT - 1), d2, 0.0)
        value += jnp.where(at == jnp.bitwise_and(to - width, FLAT - 1), d2 + q2, 0.0)
        value += jnp.where(at == base + jnp.bitwise_and(inner + 1, width - 1), d3, 0.0)
        value += jnp.where(at == base + jnp.bitwise_and(inner - 1, width - 1), d3 + q3, 0.0)
        mm[pl.ds(t * 8, 8)] = value
        return carry

    lax.fori_loop(0, FLAT // 8, neighbours, 0)
    high, low = split(mm[pl.ds(0, FLAT)])
    a_hi[...] = high
    a_lo[...] = low

    for copy in loads:
        copy.wait()

    lane_low = lax.broadcasted_iota(jnp.int32, (8, FLAT), 0) < 4
    lo_tile, hi_tile = pl.ds(0, 8), pl.ds(cy - 8, 8)

    def pack(begin, end):
        def pair(m, carry):
            even, odd = u0[2 * m, lo_tile], u0[2 * m + 1, lo_tile]
            pack_up[m] = jnp.where(lane_low, even, pltpu.roll(odd, 4, 0))
            even, odd = u0[2 * m, hi_tile], u0[2 * m + 1, hi_tile]
            pack_dn[m] = jnp.where(lane_low, pltpu.roll(odd, 4, 0), even)
            return carry

        lax.fori_loop(begin // 2, end // 2, pair, 0)

    parts = []
    for k in range(CHUNKS):
        begin = 4 if k == 0 else 8 + k * per
        end = rows + 4 if k == CHUNKS - 1 else 8 + (k + 1) * per
        parts.append((begin, end))
    pack(*parts[0])
    pack(rows, rows + 4)
    pl.semaphore_wait(barrier, len(near) + len(PEERS))

    def send(i, src, dst, device):
        copy = pltpu.make_async_remote_copy(
            src, dst, hs_sem.at[i], hr_sem.at[i], device_id=device, device_id_type=MESH
        )
        copy.start()
        return copy

    def half(begin, end):
        return pl.ds(begin // 2, (end - begin) // 2)

    body = pl.ds(0, cy)
    sides = []

    def send_side(k):
        part = half(*parts[k])
        sides.append(
            [
                send(6 + 2 * k, pack_up.at[part], up8.at[part], {"gy": gyd}),
                send(7 + 2 * k, pack_dn.at[part], dn8.at[part], {"gy": gyu}),
            ]
        )

    lasts, before = half(rows, rows + 4), half(0, 4)
    head = [
        send(0, u0.at[pl.ds(rows, 4), body], u0.at[pl.ds(0, 4), body], {"gx": gxo}),
        send(1, pack_up.at[lasts], up8.at[before], {"gx": gxo, "gy": gyd}),
        send(2, pack_dn.at[lasts], dn8.at[before], {"gx": gxo, "gy": gyu}),
    ]
    send_side(0)
    for k in range(1, CHUNKS):
        pack(parts[k][0], min(parts[k][1], rows))
        send_side(k)
    firsts, after = half(4, 8), half(rows + 4, rows + 8)
    tail = [
        send(3, u0.at[pl.ds(4, 4), body], u0.at[pl.ds(rows + 4, 4), body], {"gx": gxo}),
        send(4, pack_up.at[firsts], up8.at[after], {"gx": gxo, "gy": gyd}),
        send(5, pack_dn.at[firsts], dn8.at[after], {"gx": gxo, "gy": gyu}),
    ]

    def section(src, src_first, dst, count, final):
        def block(b, carry):
            r0 = src_first + b * 8
            flat = src[pl.ds(r0, 8)].reshape(8 * 24, FLAT)
            high, low = split(flat)
            mm[pl.ds(0, 192)] = dot(high, a_hi[...]) + dot(low, a_hi[...]) + dot(high, a_lo[...])
            for i in range(8):
                centre = src[r0 + i]
                above, below = src[r0 + i + 1], src[r0 + i - 1]
                value = (keep + rate / (1.0 + centre * centre)) * centre
                value += d0 * above + (d0 + q0) * below
                value += d1 * pltpu.roll(centre, 23, 0) + (d1 + q1) * pltpu.roll(centre, 1, 0)
                value += mm[pl.ds(i * 24, 24)]
                if final is None:
                    dst[b * 8 + i] = value
                else:
                    dst[final + b * 8 + i] = value[:cy]
            return carry

        lax.fori_loop(0, count // 8, block, 0)

    def forward(k):
        def copy(i, p, device):
            return pltpu.make_async_remote_copy(
                sent.at[pl.ds(k * per + device * own, own)],
                got.at[k, comp],
                s1.at[k, i],
                r1.at[k, i],
                device_id={"comp": device},
                device_id_type=MESH,
            )

        return [copy(i, p, mate(p)) for i, p in enumerate(PEERS)]

    def backward(k):
        def copy(i, p, device):
            return pltpu.make_async_remote_copy(
                back.at[k, device],
                out.at[pl.ds(k * per + comp * own, own)],
                s2.at[k, i],
                r2.at[k, i],
                device_id={"comp": device},
                device_id_type=MESH,
            )

        return [copy(i, p, mate(p)) for i, p in enumerate(PEERS)]

    def stencil(k):
        def halo(t, carry):
            m = k * (per // 2) + t
            up, dn = up8[m], dn8[m]
            u0[2 * m, pl.ds(cy, 8)] = jnp.where(lane_low, up, dn)
            u0[2 * m + 1, pl.ds(cy, 8)] = pltpu.roll(jnp.where(lane_low, dn, up), 4, 0)
            return carry

        lax.fori_loop(0, per // 2 + 4, halo, 0)
        section(u0, k * per + 1, ta, per + 6 + 2, None)
        section(ta, 1, tb, per + 4 + 4, None)
        section(tb, 1, ta, per + 2 + 6, None)
        section(ta, 1, sent, per, k * per)

    flat_rows = own * cy

    def place(a):
        return jnp.clip(a - LEVELS[0], 0, len(LEVELS) - 1)

    def combine(k):
        for copy in forward(k):
            copy.wait_recv()
        got[k, comp] = sent[pl.ds(k * per + comp * own, own)]
        for n, a in enumerate(LEVELS):
            total = jnp.zeros((own, cy, FLAT), jnp.float32)
            for g in range(GRIDS):
                weight = jnp.where(level_ref[g] == a, coef_ref[g], 0).astype(jnp.float32)
                total += weight * got[k, g]
            total = total.reshape(flat_rows, FLAT)
            res[n] = total
            high, low = split(total)
            lvl[n, pl.ds(0, flat_rows)] = high
            lvl[n, pl.ds(flat_rows, flat_rows)] = low
        for n, a in enumerate(LEVELS):
            value = jnp.zeros((2 * flat_rows, FLAT), jnp.float32)
            for m, other in enumerate([o for o in range(len(LEVELS)) if o != n]):
                value += dot(lvl[other], tab[n, pl.ds(m * FLAT, FLAT)])
            res[n] += value[:flat_rows] + value[flat_rows:]
        for g in range(GRIDS):
            back[k, g] = res[place(level_ref[g])].reshape(own, cy, FLAT)
        out[pl.ds(k * per + comp * own, own)] = res[place(level)].reshape(own, cy, FLAT)
        for copy in backward(k):
            copy.start()

    for k in range(CHUNKS):
        for copy in sides[k]:
            copy.wait_recv()
        if k == 0:
            for copy in head:
                copy.wait_recv()
        if k == CHUNKS - 1:
            for copy in tail:
                copy.wait_recv()
        stencil(k)
        for copy in forward(k):
            copy.start()
        if k == 0:
            tab_copy.wait()
        else:
            combine(k - 1)
    combine(CHUNKS - 1)
    for copy in head + tail + sum(sides, []):
        copy.wait_send()
    for k in range(CHUNKS):
        for copy in forward(k):
            copy.wait_send()
        for copy in backward(k):
            copy.wait()


def solution(mesh):
    table = exchange_table()

    def local(field, third_level, coefficients, rates, reaction):
        _, rows, cy, flat = field.shape
        per = rows // CHUNKS
        own = per // GRIDS
        vmem, hbm = (pl.BlockSpec(memory_space=m) for m in (pltpu.VMEM, pltpu.HBM))
        f32, bf16 = jnp.float32, jnp.bfloat16
        dma = pltpu.SemaphoreType.DMA
        peers = len(PEERS)
        halos = 6 + 2 * CHUNKS
        result = pl.pallas_call(
            kernel,
            out_shape=jax.ShapeDtypeStruct((rows, cy, flat), f32),
            in_specs=[hbm] * 6,
            out_specs=vmem,
            scratch_shapes=[
                pltpu.SMEM(third_level.shape, jnp.int32),
                pltpu.SMEM(coefficients.shape, jnp.int32),
                pltpu.SMEM(rates.shape, f32),
                pltpu.SMEM(reaction.shape, f32),
                dma((4,)),
                pltpu.VMEM((rows + 8 + 8, cy + 8, flat), f32),
                pltpu.VMEM((rows // 2 + 4, 8, flat), f32),
                pltpu.VMEM((rows // 2 + 4, 8, flat), f32),
                pltpu.VMEM((rows // 2 + 4, 8, flat), f32),
                pltpu.VMEM((rows // 2 + 4, 8, flat), f32),
                pltpu.VMEM((per + 16, cy + 8, flat), f32),
                pltpu.VMEM((per + 16, cy + 8, flat), f32),
                pltpu.VMEM((max(8 * (cy + 8), flat), flat), f32),
                pltpu.VMEM((flat, flat), bf16),
                pltpu.VMEM((flat, flat), bf16),
                pltpu.VMEM((rows, cy, flat), f32),
                pltpu.VMEM((CHUNKS, GRIDS, own, cy, flat), f32),
                pltpu.VMEM((len(LEVELS), 2 * own * cy, flat), bf16),
                pltpu.VMEM((len(LEVELS), own * cy, flat), f32),
                pltpu.VMEM((CHUNKS, GRIDS, own, cy, flat), f32),
                pltpu.VMEM(table.shape, bf16),
                dma((CHUNKS,)),
                dma,
                dma((halos,)),
                dma((halos,)),
                dma((CHUNKS, peers)),
                dma((CHUNKS, peers)),
                dma((CHUNKS, peers)),
                dma((CHUNKS, peers)),
            ],
            compiler_params=pltpu.CompilerParams(
                collective_id=0, has_side_effects=True, vmem_limit_bytes=64900000
            ),
        )(field[0], jnp.asarray(table), third_level, coefficients, rates, reaction)
        return result[None]

    return jax.shard_map(
        local,
        mesh=mesh,
        in_specs=(P("comp", "gx", "gy", None), P(), P(), P(), P()),
        out_specs=P("comp", "gx", "gy", None),
        check_vma=False,
    )
```

```python
import functools

import jax
import jax.numpy as jnp
import ml_dtypes
import numpy as np
from jax import lax
from jax.experimental import pallas as pl
from jax.experimental.pallas import tpu as pltpu
from jax.sharding import PartitionSpec as P

MESH = pl.DeviceIdType.MESH
SECTIONS = 4
LEVEL_SUM = 8
LEVELS = (2, 3, 4, 5, 6)
FLAT = 256
GRIDS = 16
BLOCK = 16
ORDER = [(1, 0), (0, 1), (3, 0), (1, 1), (2, 0), (3, 1), (2, 1)]
PEERS = [(y, z, c) for y, z in ORDER for c in (0, 1)] + [(0, 0, 1)]


def hat_matrix(fine, coarse):
    step = 2 ** (fine - coarse)
    count = 2**coarse
    out = np.zeros((2**fine, count), np.float64)
    for i in range(2**fine):
        left, part = divmod(i, step)
        out[i, left] += 1 - part / step
        out[i, (left + 1) % count] += part / step
    return out


def pick_matrix(coarse, fine):
    out = np.zeros((2**coarse, 2**fine), np.float64)
    out[np.arange(2**coarse), np.arange(2**coarse) * 2 ** (fine - coarse)] = 1
    return out


def between(low, high):
    return pick_matrix(low, high) if low <= high else hat_matrix(low, high)


def exchange_matrix(to, source):
    third = between(to, source)
    fourth = between(LEVEL_SUM - to, LEVEL_SUM - source)
    return np.kron(third, fourth).T


def exchange_table():
    out = np.stack(
        [
            np.concatenate([exchange_matrix(to, source) for source in LEVELS if source != to])
            for to in LEVELS
        ]
    )
    return out.astype(ml_dtypes.bfloat16)


def split(values):
    high = values.astype(jnp.bfloat16)
    return high, (values - high.astype(jnp.float32)).astype(jnp.bfloat16)


def dot(a, b):
    return jnp.dot(a, b, preferred_element_type=jnp.float32)


def kernel(
    field, table, level_in, coef_in, rate_in, react_in,
    land,
    level_ref, coef_ref, rate_ref, react_ref, small_sem,
    u0, pack_up, pack_dn, up8, dn8, ta, tb, mm, a_hi, a_lo, sent, got, lvl, res, back, mine, mine_sem, tab,
    load_sem, tab_sem, hs_sem, hr_sem, s1, r1, s2, r2,
):
    rows, cy = field.shape[0], field.shape[1]
    per = rows // 2
    own = per // GRIDS
    comp, gx, gy = (lax.axis_index(a) for a in ("comp", "gx", "gy"))
    y, z, c = comp // 4, (comp // 2) % 2, comp % 2

    def mate(p, sign=1):
        return ((y + sign * p[0]) % 4) * 4 + ((z + p[1]) % 2) * 2 + (c + p[2]) % 2

    quarter = rows // 4
    loads = [
        pltpu.make_async_copy(
            field.at[pl.ds(k * quarter, quarter)],
            u0.at[pl.ds(4 + k * quarter, quarter), pl.ds(0, cy)],
            load_sem.at[k],
        )
        for k in range(4)
    ]
    smalls = [
        pltpu.make_async_copy(src, dst, small_sem.at[i])
        for i, (src, dst) in enumerate(
            [(level_in, level_ref), (rate_in, rate_ref), (react_in, react_ref), (coef_in, coef_ref)]
        )
    ]
    for copy in smalls + loads:
        copy.start()
    tab_copy = pltpu.make_async_copy(table, tab, tab_sem)
    tab_copy.start()

    gxo = (gx + 1) % 2
    gyu, gyd = (gy + 1) % 4, (gy + 3) % 4
    near = [
        {"gx": gxo},
        {"gy": gyu},
        {"gy": gyd},
        {"gx": gxo, "gy": gyu},
        {"gx": gxo, "gy": gyd},
    ]
    barrier = pltpu.get_barrier_semaphore()
    for device in near + [{"comp": mate(p)} for p in PEERS]:
        pl.semaphore_signal(barrier, inc=1, device_id=device, device_id_type=MESH)

    for copy in smalls:
        copy.wait()
    level = level_ref[comp]
    coarse3 = jnp.float32(1.0)
    coarse4 = jnp.float32(1.0)
    for a in LEVELS:
        coarse3 = jnp.where(level == a, jnp.float32(2.0 ** (a - 6)), coarse3)
        coarse4 = jnp.where(level == a, jnp.float32(2.0 ** (2 - a)), coarse4)
    d0, d1 = rate_ref[0, 0], rate_ref[0, 1]
    d2, d3 = rate_ref[0, 2] * (coarse3 * coarse3), rate_ref[0, 3] * (coarse4 * coarse4)
    q0, q1 = rate_ref[1, 0], rate_ref[1, 1]
    q2, q3 = rate_ref[1, 2] * coarse3, rate_ref[1, 3] * coarse4
    rate = react_ref[0]
    keep = 1.0 - 2.0 * (d0 + d1 + d2 + d3) - (q0 + q1 + q2 + q3)
    width = jnp.int32(1)
    for a in LEVELS:
        width = jnp.where(level == a, jnp.int32(2 ** (LEVEL_SUM - a)), width)

    def neighbours(t, carry):
        at = t * 16 + lax.broadcasted_iota(jnp.int32, (16, FLAT), 0)
        to = lax.broadcasted_iota(jnp.int32, (16, FLAT), 1)
        inner = jnp.bitwise_and(to, width - 1)
        base = to - inner
        value = jnp.where(at == jnp.bitwise_and(to + width, FLAT - 1), d2, 0.0)
        value += jnp.where(at == jnp.bitwise_and(to - width, FLAT - 1), d2 + q2, 0.0)
        value += jnp.where(at == base + jnp.bitwise_and(inner + 1, width - 1), d3, 0.0)
        value += jnp.where(at == base + jnp.bitwise_and(inner - 1, width - 1), d3 + q3, 0.0)
        high, low = split(value)
        part = pl.ds(pl.multiple_of(t * 16, 16), 16)
        a_hi[part] = high
        a_lo[part] = low
        return carry

    lax.fori_loop(0, FLAT // 16, neighbours, 0)
    for copy in loads:
        copy.wait()

    def section(src, src_first, dst, dst_first, count, size, tall, final):
        kept = cy if final else tall
        flat = size * kept

        def block(b, carry):
            r0 = src_first + b * size
            high, low = split(src[pl.ds(r0, size), pl.ds(0, kept)].reshape(flat, FLAT))
            both = dot(jnp.concatenate([high, low]), a_hi[...])
            mm[pl.ds(0, flat)] = both[:flat] + both[flat:] + dot(high, a_lo[...])
            for i in range(size):
                whole = src[r0 + i, pl.ds(0, tall)]
                centre = whole[:kept]
                above, below = src[r0 + i + 1, pl.ds(0, kept)], src[r0 + i - 1, pl.ds(0, kept)]
                value = (keep + rate / (1.0 + centre * centre)) * centre
                value += d0 * above + (d0 + q0) * below
                value += d1 * pltpu.roll(whole, tall - 1, 0)[:kept]
                value += (d1 + q1) * pltpu.roll(whole, 1, 0)[:kept]
                value += mm[pl.ds(i * kept, kept)]
                if final == "inner":
                    low4, high4 = pltpu.roll(value[:8], 4, 0), pltpu.roll(value[8:16], 4, 0)
                    value = jnp.where(lane_low, low4, high4)
                elif final == "outer":
                    value = jnp.where(lane_low, value[:8], value[8:16])
                if final is None:
                    dst[dst_first + b * size + i, pl.ds(0, tall)] = value
                else:
                    dst[dst_first + b * size + i] = value
            return carry

        lax.fori_loop(0, count // size, block, 0)

    lane_low = lax.broadcasted_iota(jnp.int32, (8, FLAT), 0) < 4
    lo_tile, hi_tile = pl.ds(0, 8), pl.ds(cy - 8, 8)

    def early(first, count, tall):
        size = next(n for n in range(14, 32) if (count + 6) % n == 0)
        section(u0, first + 1, ta, 0, count + 6, size, tall, None)
        section(ta, 1, tb, 0, count + 6, size, tall, None)
        section(tb, 1, ta, 0, count + 6, size, tall, None)

    def late(count, tall, final, at):
        section(ta, 1, sent, at, count, BLOCK, tall, final)

    def pack(m, carry):
        even, odd = u0[2 * m, lo_tile], u0[2 * m + 1, lo_tile]
        pack_up[m] = jnp.where(lane_low, even, pltpu.roll(odd, 4, 0))
        even, odd = u0[2 * m, hi_tile], u0[2 * m + 1, hi_tile]
        pack_dn[m] = jnp.where(lane_low, pltpu.roll(odd, 4, 0), even)
        return carry

    lax.fori_loop(2, rows // 2 + 2, pack, 0)

    def send(i, src, dst, device):
        return pltpu.make_async_remote_copy(
            src, dst, hs_sem.at[i], hr_sem.at[i], device_id=device, device_id_type=MESH
        )

    def half(begin, end):
        return pl.ds(begin // 2, (end - begin) // 2)

    body = pl.ds(0, cy)
    lasts, before = half(rows, rows + 4), half(0, 4)
    firsts, after = half(4, 8), half(rows + 4, rows + 8)
    rims = [
        send(0, u0.at[pl.ds(rows, 4), body], u0.at[pl.ds(0, 4), body], {"gx": gxo}),
        send(3, u0.at[pl.ds(4, 4), body], u0.at[pl.ds(rows + 4, 4), body], {"gx": gxo}),
    ]
    corners = [
        send(1, pack_up.at[lasts], up8.at[before], {"gx": gxo, "gy": gyd}),
        send(2, pack_dn.at[lasts], dn8.at[before], {"gx": gxo, "gy": gyu}),
        send(4, pack_up.at[firsts], up8.at[after], {"gx": gxo, "gy": gyd}),
        send(5, pack_dn.at[firsts], dn8.at[after], {"gx": gxo, "gy": gyu}),
    ]
    sides = []
    for k, (begin, end) in enumerate([(4, per + 8), (per + 8, rows + 4)]):
        part = half(begin, end)
        sides.append(
            [
                send(6 + 2 * k, pack_up.at[part], up8.at[part], {"gy": gyd}),
                send(7 + 2 * k, pack_dn.at[part], dn8.at[part], {"gy": gyu}),
            ]
        )

    def forward(k):
        def copy(i, device):
            return pltpu.make_async_remote_copy(
                sent.at[pl.ds(k * per + device * own, own)],
                got.at[k, comp],
                s1.at[k, i],
                r1.at[k, i],
                device_id={"comp": device},
                device_id_type=MESH,
            )

        return [copy(i, mate(p)) for i, p in enumerate(PEERS)]

    def backward(k):
        def copy(i, device):
            return pltpu.make_async_remote_copy(
                back.at[k, device],
                land.at[pl.ds(k * per + comp * own, own)],
                s2.at[k, i],
                r2.at[k, i],
                device_id={"comp": device},
                device_id_type=MESH,
            )

        return [copy(i, mate(p)) for i, p in enumerate(PEERS)]

    flat_rows = own * 8

    def place(a):
        return jnp.clip(a - LEVELS[0], 0, len(LEVELS) - 1)

    def own_copy(k):
        return pltpu.make_async_copy(
            mine.at[k], land.at[pl.ds(k * per + comp * own, own)], mine_sem.at[k]
        )

    def combine(k):
        for copy in forward(k):
            copy.wait_recv()
        got[k, comp] = sent[pl.ds(k * per + comp * own, own)]
        for n, a in enumerate(LEVELS):
            total = jnp.zeros((own, 8, FLAT), jnp.float32)
            for g in range(GRIDS):
                weight = jnp.where(level_ref[g] == a, coef_ref[g], 0).astype(jnp.float32)
                total += weight * got[k, g]
            total = total.reshape(flat_rows, FLAT)
            res[n] = total
            high, low = split(total)
            lvl[n, pl.ds(0, flat_rows)] = high
            lvl[n, pl.ds(flat_rows, flat_rows)] = low
        for n, a in enumerate(LEVELS):
            value = jnp.zeros((2 * flat_rows, FLAT), jnp.float32)
            for m, other in enumerate([o for o in range(len(LEVELS)) if o != n]):
                value += dot(lvl[other], tab[n, pl.ds(m * FLAT, FLAT)])
            res[n] += value[:flat_rows] + value[flat_rows:]
        for g in range(GRIDS):
            back[k, g] = res[place(level_ref[g])].reshape(own, 8, FLAT)
        mine[k] = res[place(level)].reshape(own, 8, FLAT)
        own_copy(k).start()
        for copy in backward(k):
            copy.start()

    def stencil_outer(k):
        def halo(t, carry):
            m = k * (per // 2) + t
            up, dn = up8[m], dn8[m]
            u0[2 * m, pl.ds(cy, 8)] = jnp.where(lane_low, up, dn)
            u0[2 * m + 1, pl.ds(cy, 8)] = pltpu.roll(jnp.where(lane_low, dn, up), 4, 0)
            return carry

        lax.fori_loop(0, per // 2 + 4, halo, 0)
        early(k * per, per, cy + 8)
        late(per, cy + 8, "outer", (2 + k) * per)

    def start(copies):
        for copy in copies:
            copy.start()

    early(quarter, per, cy)
    pl.semaphore_wait(barrier, len(near) + len(PEERS))
    start(rims + sides[0] + corners + sides[1])
    late(per, cy, "inner", 0)
    start(forward(0))
    for copy in rims:
        copy.wait_recv()
    for n, first in enumerate((3 * quarter, 0)):
        early(first, quarter, cy)
        late(quarter, cy, "inner", per + n * quarter)
    start(forward(1))
    tab_copy.wait()
    for copy in sides[0] + corners:
        copy.wait_recv()
    combine(0)
    stencil_outer(0)
    start(forward(2))
    combine(1)
    for copy in sides[1]:
        copy.wait_recv()
    stencil_outer(1)
    start(forward(3))
    combine(2)
    combine(3)
    for copy in rims + corners + sides[0] + sides[1]:
        copy.wait_send()
    for k in range(4):
        for copy in forward(k):
            copy.wait_send()
        for copy in backward(k):
            copy.wait()
        own_copy(k).wait()


def finish(outer, inner, out):
    lane_low = lax.broadcasted_iota(jnp.int32, (8, FLAT), 0) < 4
    for x in range(outer.shape[0]):
        turned = pltpu.roll(inner[x], 4, 0)
        out[x, pl.ds(0, 8)] = jnp.where(lane_low, outer[x], turned)
        out[x, pl.ds(8, 8)] = jnp.where(lane_low, turned, outer[x])


def solution(mesh):
    table = exchange_table()

    def local(field, third_level, coefficients, rates, reaction):
        _, rows, cy, flat = field.shape
        per = rows // 2
        own = per // GRIDS
        tall = cy + 8
        height = per + 32
        hbm = pl.BlockSpec(memory_space=pltpu.HBM)
        f32, bf16 = jnp.float32, jnp.bfloat16
        dma = pltpu.SemaphoreType.DMA
        peers = len(PEERS)
        halos = 10
        landed = pl.pallas_call(
            kernel,
            out_shape=jax.ShapeDtypeStruct((2 * rows, 8, flat), f32),
            in_specs=[hbm] * 6,
            out_specs=hbm,
            scratch_shapes=[
                pltpu.SMEM(third_level.shape, jnp.int32),
                pltpu.SMEM(coefficients.shape, jnp.int32),
                pltpu.SMEM(rates.shape, f32),
                pltpu.SMEM(reaction.shape, f32),
                dma((4,)),
                pltpu.VMEM((rows + 24, tall, flat), f32),
                pltpu.VMEM((rows // 2 + 4, 8, flat), f32),
                pltpu.VMEM((rows // 2 + 4, 8, flat), f32),
                pltpu.VMEM((rows // 2 + 4, 8, flat), f32),
                pltpu.VMEM((rows // 2 + 4, 8, flat), f32),
                pltpu.VMEM((height, tall, flat), f32),
                pltpu.VMEM((height, tall, flat), f32),
                pltpu.VMEM((32 * tall, flat), f32),
                pltpu.VMEM((flat, flat), bf16),
                pltpu.VMEM((flat, flat), bf16),
                pltpu.VMEM((2 * rows, 8, flat), f32),
                pltpu.VMEM((4, GRIDS, own, 8, flat), f32),
                pltpu.VMEM((len(LEVELS), 2 * own * 8, flat), bf16),
                pltpu.VMEM((len(LEVELS), own * 8, flat), f32),
                pltpu.VMEM((4, GRIDS, own, 8, flat), f32),
                pltpu.VMEM((4, own, 8, flat), f32),
                dma((4,)),
                pltpu.VMEM(table.shape, bf16),
                dma((4,)),
                dma,
                dma((halos,)),
                dma((halos,)),
                dma((4, peers)),
                dma((4, peers)),
                dma((4, peers)),
                dma((4, peers)),
            ],
            compiler_params=pltpu.CompilerParams(
                collective_id=0, has_side_effects=True, vmem_limit_bytes=64900000
            ),
        )(field[0], jnp.asarray(table), third_level, coefficients, rates, reaction)
        step = rows // 4
        result = pl.pallas_call(
            finish,
            out_shape=jax.ShapeDtypeStruct((rows, cy, flat), f32),
            grid=(4,),
            in_specs=[
                pl.BlockSpec((step, 8, flat), lambda i: (4 + i, 0, 0)),
                pl.BlockSpec((step, 8, flat), lambda i: ((i + 3) % 4, 0, 0)),
            ],
            out_specs=pl.BlockSpec((step, cy, flat), lambda i: (i, 0, 0)),
        )(landed, landed)
        return result[None]

    return jax.shard_map(
        local,
        mesh=mesh,
        in_specs=(P("comp", "gx", "gy", None), P(), P(), P(), P()),
        out_specs=P("comp", "gx", "gy", None),
        check_vma=False,
    )
```

```python
import functools

import jax
import jax.numpy as jnp
import ml_dtypes
import numpy as np
from jax import lax
from jax.experimental import pallas as pl
from jax.experimental.pallas import tpu as pltpu
from jax.sharding import PartitionSpec as P

MESH = pl.DeviceIdType.MESH
SECTIONS = 4
LEVEL_SUM = 8
LEVELS = (2, 3, 4, 5, 6)
FLAT = 256
GRIDS = 16
BLOCK = 32
ORDER = [(1, 0), (0, 1), (3, 0), (1, 1), (2, 0), (3, 1), (2, 1)]
PEERS = [(y, z, c) for y, z in ORDER for c in (0, 1)] + [(0, 0, 1)]


def hat_matrix(fine, coarse):
    step = 2 ** (fine - coarse)
    count = 2**coarse
    out = np.zeros((2**fine, count), np.float64)
    for i in range(2**fine):
        left, part = divmod(i, step)
        out[i, left] += 1 - part / step
        out[i, (left + 1) % count] += part / step
    return out


def pick_matrix(coarse, fine):
    out = np.zeros((2**coarse, 2**fine), np.float64)
    out[np.arange(2**coarse), np.arange(2**coarse) * 2 ** (fine - coarse)] = 1
    return out


def between(low, high):
    return pick_matrix(low, high) if low <= high else hat_matrix(low, high)


def exchange_matrix(to, source):
    third = between(to, source)
    fourth = between(LEVEL_SUM - to, LEVEL_SUM - source)
    return np.kron(third, fourth).T


def exchange_table():
    out = np.stack(
        [
            np.concatenate([exchange_matrix(to, source) for source in LEVELS if source != to])
            for to in LEVELS
        ]
    )
    return out.astype(ml_dtypes.bfloat16)


def split(values):
    high = values.astype(jnp.bfloat16)
    return high, (values - high.astype(jnp.float32)).astype(jnp.bfloat16)


def dot(a, b):
    return jnp.dot(a, b, preferred_element_type=jnp.float32)


def kernel(
    field, table, level_in, coef_in, rate_in, react_in,
    land,
    level_ref, coef_ref, rate_ref, react_ref, small_sem,
    u0, pack_up, pack_dn, up8, dn8, ta, tb, mm, a_hi, a_lo, sent, got, lvl, res, back, mine, mine_sem, tab,
    load_sem, tab_sem, hs_sem, hr_sem, s1, r1, s2, r2,
):
    rows, cy = field.shape[0], field.shape[1]
    per = rows // 2
    own = per // GRIDS
    comp, gx, gy = (lax.axis_index(a) for a in ("comp", "gx", "gy"))
    y, z, c = comp // 4, (comp // 2) % 2, comp % 2

    def mate(p, sign=1):
        return ((y + sign * p[0]) % 4) * 4 + ((z + p[1]) % 2) * 2 + (c + p[2]) % 2

    quarter = rows // 4
    loads = [
        pltpu.make_async_copy(
            field.at[pl.ds(k * quarter, quarter)],
            u0.at[pl.ds(4 + k * quarter, quarter), pl.ds(0, cy)],
            load_sem.at[k],
        )
        for k in range(4)
    ]
    smalls = [
        pltpu.make_async_copy(src, dst, small_sem.at[i])
        for i, (src, dst) in enumerate(
            [(level_in, level_ref), (rate_in, rate_ref), (react_in, react_ref), (coef_in, coef_ref)]
        )
    ]
    for copy in smalls + loads:
        copy.start()
    tab_copy = pltpu.make_async_copy(table, tab, tab_sem)
    tab_copy.start()

    gxo = (gx + 1) % 2
    gyu, gyd = (gy + 1) % 4, (gy + 3) % 4
    near = [
        {"gx": gxo},
        {"gy": gyu},
        {"gy": gyd},
        {"gx": gxo, "gy": gyu},
        {"gx": gxo, "gy": gyd},
    ]
    barrier = pltpu.get_barrier_semaphore()
    for device in near + [{"comp": mate(p)} for p in PEERS]:
        pl.semaphore_signal(barrier, inc=1, device_id=device, device_id_type=MESH)

    for copy in smalls:
        copy.wait()
    level = level_ref[comp]
    coarse3 = jnp.float32(1.0)
    coarse4 = jnp.float32(1.0)
    for a in LEVELS:
        coarse3 = jnp.where(level == a, jnp.float32(2.0 ** (a - 6)), coarse3)
        coarse4 = jnp.where(level == a, jnp.float32(2.0 ** (2 - a)), coarse4)
    d0, d1 = rate_ref[0, 0], rate_ref[0, 1]
    d2, d3 = rate_ref[0, 2] * (coarse3 * coarse3), rate_ref[0, 3] * (coarse4 * coarse4)
    q0, q1 = rate_ref[1, 0], rate_ref[1, 1]
    q2, q3 = rate_ref[1, 2] * coarse3, rate_ref[1, 3] * coarse4
    rate = react_ref[0]
    keep = 1.0 - 2.0 * (d0 + d1 + d2 + d3) - (q0 + q1 + q2 + q3)
    width = jnp.int32(1)
    for a in LEVELS:
        width = jnp.where(level == a, jnp.int32(2 ** (LEVEL_SUM - a)), width)

    def neighbours(t, carry):
        at = t * 16 + lax.broadcasted_iota(jnp.int32, (16, FLAT), 0)
        to = lax.broadcasted_iota(jnp.int32, (16, FLAT), 1)
        inner = jnp.bitwise_and(to, width - 1)
        base = to - inner
        value = jnp.where(at == jnp.bitwise_and(to + width, FLAT - 1), d2, 0.0)
        value += jnp.where(at == jnp.bitwise_and(to - width, FLAT - 1), d2 + q2, 0.0)
        value += jnp.where(at == base + jnp.bitwise_and(inner + 1, width - 1), d3, 0.0)
        value += jnp.where(at == base + jnp.bitwise_and(inner - 1, width - 1), d3 + q3, 0.0)
        high, low = split(value)
        part = pl.ds(pl.multiple_of(t * 16, 16), 16)
        a_hi[part] = high
        a_lo[part] = low
        return carry

    lax.fori_loop(0, FLAT // 16, neighbours, 0)
    for copy in loads:
        copy.wait()

    def section(src, src_first, dst, dst_first, count, size, tall, final):
        kept = cy if final else tall
        flat = size * kept

        def block(b, carry):
            r0 = src_first + b * size
            high, low = split(src[pl.ds(r0, size), pl.ds(0, kept)].reshape(flat, FLAT))
            both = dot(jnp.concatenate([high, low]), a_hi[...])
            mm[pl.ds(0, flat)] = both[:flat] + both[flat:] + dot(high, a_lo[...])
            for i in range(size):
                whole = src[r0 + i, pl.ds(0, tall)]
                centre = whole[:kept]
                above, below = src[r0 + i + 1, pl.ds(0, kept)], src[r0 + i - 1, pl.ds(0, kept)]
                value = (keep + rate / (1.0 + centre * centre)) * centre
                value += d0 * above + (d0 + q0) * below
                value += d1 * pltpu.roll(whole, tall - 1, 0)[:kept]
                value += (d1 + q1) * pltpu.roll(whole, 1, 0)[:kept]
                value += mm[pl.ds(i * kept, kept)]
                if final == "inner":
                    low4, high4 = pltpu.roll(value[:8], 4, 0), pltpu.roll(value[8:16], 4, 0)
                    value = jnp.where(lane_low, low4, high4)
                elif final == "outer":
                    value = jnp.where(lane_low, value[:8], value[8:16])
                if final is None:
                    dst[dst_first + b * size + i, pl.ds(0, tall)] = value
                else:
                    dst[dst_first + b * size + i] = value
            return carry

        lax.fori_loop(0, count // size, block, 0)

    lane_low = lax.broadcasted_iota(jnp.int32, (8, FLAT), 0) < 4
    lo_tile, hi_tile = pl.ds(0, 8), pl.ds(cy - 8, 8)

    def early(first, count, tall):
        size = next(n for n in range(14, 32) if (count + 6) % n == 0)
        section(u0, first + 1, ta, 0, count + 6, size, tall, None)
        section(ta, 1, tb, 0, count + 6, size, tall, None)
        section(tb, 1, ta, 0, count + 6, size, tall, None)

    def late(count, tall, final, at):
        section(ta, 1, sent, at, count, BLOCK, tall, final)

    def pack(m, carry):
        even, odd = u0[2 * m, lo_tile], u0[2 * m + 1, lo_tile]
        pack_up[m] = jnp.where(lane_low, even, pltpu.roll(odd, 4, 0))
        even, odd = u0[2 * m, hi_tile], u0[2 * m + 1, hi_tile]
        pack_dn[m] = jnp.where(lane_low, pltpu.roll(odd, 4, 0), even)
        return carry

    lax.fori_loop(2, rows // 2 + 2, pack, 0)

    def send(i, src, dst, device):
        return pltpu.make_async_remote_copy(
            src, dst, hs_sem.at[i], hr_sem.at[i], device_id=device, device_id_type=MESH
        )

    def half(begin, end):
        return pl.ds(begin // 2, (end - begin) // 2)

    body = pl.ds(0, cy)
    lasts, before = half(rows, rows + 4), half(0, 4)
    firsts, after = half(4, 8), half(rows + 4, rows + 8)
    rims = [
        send(0, u0.at[pl.ds(rows, 4), body], u0.at[pl.ds(0, 4), body], {"gx": gxo}),
        send(3, u0.at[pl.ds(4, 4), body], u0.at[pl.ds(rows + 4, 4), body], {"gx": gxo}),
    ]
    corners = [
        send(1, pack_up.at[lasts], up8.at[before], {"gx": gxo, "gy": gyd}),
        send(2, pack_dn.at[lasts], dn8.at[before], {"gx": gxo, "gy": gyu}),
        send(4, pack_up.at[firsts], up8.at[after], {"gx": gxo, "gy": gyd}),
        send(5, pack_dn.at[firsts], dn8.at[after], {"gx": gxo, "gy": gyu}),
    ]
    sides = []
    for k, (begin, end) in enumerate([(4, per + 8), (per + 8, rows + 4)]):
        part = half(begin, end)
        sides.append(
            [
                send(6 + 2 * k, pack_up.at[part], up8.at[part], {"gy": gyd}),
                send(7 + 2 * k, pack_dn.at[part], dn8.at[part], {"gy": gyu}),
            ]
        )

    def forward(k):
        def copy(i, device):
            return pltpu.make_async_remote_copy(
                sent.at[pl.ds(k * per + device * own, own)],
                got.at[k, comp],
                s1.at[k, i],
                r1.at[k, i],
                device_id={"comp": device},
                device_id_type=MESH,
            )

        return [copy(i, mate(p)) for i, p in enumerate(PEERS)]

    def backward(k):
        def copy(i, device):
            return pltpu.make_async_remote_copy(
                back.at[k, device],
                land.at[pl.ds(k * per + comp * own, own)],
                s2.at[k, i],
                r2.at[k, i],
                device_id={"comp": device},
                device_id_type=MESH,
            )

        return [copy(i, mate(p)) for i, p in enumerate(PEERS)]

    flat_rows = own * 8

    def place(a):
        return jnp.clip(a - LEVELS[0], 0, len(LEVELS) - 1)

    def own_copy(k):
        return pltpu.make_async_copy(
            mine.at[k], land.at[pl.ds(k * per + comp * own, own)], mine_sem.at[k]
        )

    def combine(k):
        for copy in forward(k):
            copy.wait_recv()
        got[k, comp] = sent[pl.ds(k * per + comp * own, own)]
        for n, a in enumerate(LEVELS):
            total = jnp.zeros((own, 8, FLAT), jnp.float32)
            for g in range(GRIDS):
                weight = jnp.where(level_ref[g] == a, coef_ref[g], 0).astype(jnp.float32)
                total += weight * got[k, g]
            total = total.reshape(flat_rows, FLAT)
            res[n] = total
            high, low = split(total)
            lvl[n, pl.ds(0, flat_rows)] = high
            lvl[n, pl.ds(flat_rows, flat_rows)] = low
        for n, a in enumerate(LEVELS):
            value = jnp.zeros((2 * flat_rows, FLAT), jnp.float32)
            for m, other in enumerate([o for o in range(len(LEVELS)) if o != n]):
                value += dot(lvl[other], tab[n, pl.ds(m * FLAT, FLAT)])
            res[n] += value[:flat_rows] + value[flat_rows:]
        for g in range(GRIDS):
            back[k, g] = res[place(level_ref[g])].reshape(own, 8, FLAT)
        mine[k] = res[place(level)].reshape(own, 8, FLAT)
        own_copy(k).start()
        for copy in backward(k):
            copy.start()

    def stencil_outer(k):
        def halo(t, carry):
            m = k * (per // 2) + t
            up, dn = up8[m], dn8[m]
            u0[2 * m, pl.ds(cy, 8)] = jnp.where(lane_low, up, dn)
            u0[2 * m + 1, pl.ds(cy, 8)] = pltpu.roll(jnp.where(lane_low, dn, up), 4, 0)
            return carry

        lax.fori_loop(0, per // 2 + 4, halo, 0)
        early(k * per, per, cy + 8)
        late(per, cy + 8, "outer", (2 + k) * per)

    def start(copies):
        for copy in copies:
            copy.start()

    early(quarter, per, cy)
    pl.semaphore_wait(barrier, len(near) + len(PEERS))
    start(rims + sides[0] + corners + sides[1])
    late(per, cy, "inner", 0)
    start(forward(0))
    for copy in rims:
        copy.wait_recv()
    for n, first in enumerate((3 * quarter, 0)):
        early(first, quarter, cy)
        late(quarter, cy, "inner", per + n * quarter)
    start(forward(1))
    tab_copy.wait()
    for copy in sides[0] + corners:
        copy.wait_recv()
    combine(0)
    stencil_outer(0)
    start(forward(2))
    combine(1)
    for copy in sides[1]:
        copy.wait_recv()
    stencil_outer(1)
    start(forward(3))
    combine(2)
    combine(3)
    for copy in rims + corners + sides[0] + sides[1]:
        copy.wait_send()
    for k in range(4):
        for copy in forward(k):
            copy.wait_send()
        for copy in backward(k):
            copy.wait()
        own_copy(k).wait()


def finish(landed, result, held, done, in_sem, out_sem):
    rows = result.shape[0]
    step = rows // 4
    lane_low = lax.broadcasted_iota(jnp.int32, (8, FLAT), 0) < 4

    def bring(i):
        part = pl.ds(i * step, step)
        return pltpu.make_async_copy(landed.at[part], held.at[part], in_sem.at[i])

    def put(i):
        part = pl.ds(i * step, step)
        return pltpu.make_async_copy(done.at[part], result.at[part], out_sem.at[i])

    for i in range(4):
        bring(4 + i).start()
        bring((i + 3) % 4).start()
    for i in range(4):
        bring(4 + i).wait()
        bring((i + 3) % 4).wait()

        def rows_of(t, carry):
            for n in range(4):
                x = t * 4 + n
                outer = held[rows + i * step + x]
                turned = pltpu.roll(held[(i + 3) % 4 * step + x], 4, 0)
                done[i * step + x, pl.ds(0, 8)] = jnp.where(lane_low, outer, turned)
                done[i * step + x, pl.ds(8, 8)] = jnp.where(lane_low, turned, outer)
            return carry

        lax.fori_loop(0, step // 4, rows_of, 0)
        put(i).start()
    for i in range(4):
        put(i).wait()


def solution(mesh):
    table = exchange_table()

    def local(field, third_level, coefficients, rates, reaction):
        _, rows, cy, flat = field.shape
        per = rows // 2
        own = per // GRIDS
        tall = cy + 8
        height = per + 32
        hbm = pl.BlockSpec(memory_space=pltpu.HBM)
        f32, bf16 = jnp.float32, jnp.bfloat16
        dma = pltpu.SemaphoreType.DMA
        peers = len(PEERS)
        halos = 10
        landed = pl.pallas_call(
            kernel,
            out_shape=jax.ShapeDtypeStruct((2 * rows, 8, flat), f32),
            in_specs=[hbm] * 6,
            out_specs=hbm,
            scratch_shapes=[
                pltpu.SMEM(third_level.shape, jnp.int32),
                pltpu.SMEM(coefficients.shape, jnp.int32),
                pltpu.SMEM(rates.shape, f32),
                pltpu.SMEM(reaction.shape, f32),
                dma((4,)),
                pltpu.VMEM((rows + 24, tall, flat), f32),
                pltpu.VMEM((rows // 2 + 4, 8, flat), f32),
                pltpu.VMEM((rows // 2 + 4, 8, flat), f32),
                pltpu.VMEM((rows // 2 + 4, 8, flat), f32),
                pltpu.VMEM((rows // 2 + 4, 8, flat), f32),
                pltpu.VMEM((height, tall, flat), f32),
                pltpu.VMEM((height, tall, flat), f32),
                pltpu.VMEM((32 * tall, flat), f32),
                pltpu.VMEM((flat, flat), bf16),
                pltpu.VMEM((flat, flat), bf16),
                pltpu.VMEM((2 * rows, 8, flat), f32),
                pltpu.VMEM((4, GRIDS, own, 8, flat), f32),
                pltpu.VMEM((len(LEVELS), 2 * own * 8, flat), bf16),
                pltpu.VMEM((len(LEVELS), own * 8, flat), f32),
                pltpu.VMEM((4, GRIDS, own, 8, flat), f32),
                pltpu.VMEM((4, own, 8, flat), f32),
                dma((4,)),
                pltpu.VMEM(table.shape, bf16),
                dma((4,)),
                dma,
                dma((halos,)),
                dma((halos,)),
                dma((4, peers)),
                dma((4, peers)),
                dma((4, peers)),
                dma((4, peers)),
            ],
            compiler_params=pltpu.CompilerParams(
                collective_id=0, has_side_effects=True, vmem_limit_bytes=64900000
            ),
        )(field[0], jnp.asarray(table), third_level, coefficients, rates, reaction)
        result = pl.pallas_call(
            finish,
            out_shape=jax.ShapeDtypeStruct((rows, cy, flat), f32),
            in_specs=[hbm],
            out_specs=hbm,
            scratch_shapes=[
                pltpu.VMEM((2 * rows, 8, flat), f32),
                pltpu.VMEM((rows, cy, flat), f32),
                dma((8,)),
                dma((4,)),
            ],
            compiler_params=pltpu.CompilerParams(vmem_limit_bytes=64900000),
        )(landed)
        return result[None]

    return jax.shard_map(
        local,
        mesh=mesh,
        in_specs=(P("comp", "gx", "gy", None), P(), P(), P(), P()),
        out_specs=P("comp", "gx", "gy", None),
        check_vma=False,
    )
```
